32 devices in a mesh: seq: 8 (over z, y), grp: 4 (over x, core).
Axes of the slice: x: 2, y: 2, z: 4, core: 2. Of those that a mesh axis runs over, the one named last changes fastest.
Arguments:
- doc_lengths: int32 [4, 4], P('grp'), may hold values from 1 to 512, 1024 in all within a row
- hidden: bfloat16 [4, 1024, 7168], P('grp', 'seq'), may hold values from -6 to 6
- gate_weight: bfloat16 [7168, 64], P(('seq', 'grp')), may hold values from -0.0625 to 0.0625
- target_query: bfloat16 [4, 1024, 36864], P('grp', 'seq'), may hold values from -30 to 30
- latent_keys: bfloat16 [4, 1024, 576], P('grp', 'seq'), may hold values from -6 to 6
- index_query: bfloat16 [4, 1024, 8192], P('grp', 'seq'), may hold values from -15 to 15
- index_keys: bfloat16 [4, 1024, 128], P('grp', 'seq'), may hold values from -6 to 6
Outputs:
- divergence: float32 [4, 1024], P('grp', 'seq')
- grad_gate: float32 [7168, 64], P(('seq', 'grp'))
The draws below stay inside these ranges and needn't reach their ends.
All inputs are finite; a program needn't handle non-finite values.
Results may differ from the reference program's by a relative error of at most 0.0022.
Values may be sent and summed in bfloat16 or wider, within the bound.
No kernel may reach another device: no remote copies, remote signals or barrier semaphores. Data moves between devices by JAX's collectives and lax.ppermute only.
A program may use at most 128 MiB of HBM per device.

```python
import math
import jax
import jax.numpy as jnp
import numpy as np
from jax import lax

D = 7168
HI = 64
DI = 128
HT = 64
RK = 576
TOK_DEV = 128
GROUPS = 4
TOKG = 1024
DOC_MOST = 512
WIN = 640
DOCS = 4
N_SEQ = 8


def latent_base(key):
    return jnp.clip(jax.random.normal(jax.random.fold_in(key, 101), (GROUPS, TOKG, RK), jnp.float32), -6.0, 6.0)


def index_base(key):
    return jnp.clip(jax.random.normal(jax.random.fold_in(key, 201), (GROUPS, TOKG, DI), jnp.float32), -6.0, 6.0)


def draw_latent_keys(key, part):
    return latent_base(key).astype(jnp.bfloat16)


def draw_index_keys(key, part):
    return index_base(key).astype(jnp.bfloat16)


def draw_target_query(key, part):
    values = jnp.clip(jax.random.normal(jax.random.fold_in(key, 102), (GROUPS, TOKG, HT, RK), jnp.float32), -6.0, 6.0)
    return jnp.clip(values, -30.0, 30.0).reshape(GROUPS, TOKG, HT * RK).astype(jnp.bfloat16)


def draw_index_query(key, part):
    values = 0.5 * jnp.clip(jax.random.normal(jax.random.fold_in(key, 202), (GROUPS, TOKG, HI, DI), jnp.float32), -6.0, 6.0)
    return jnp.clip(values, -15.0, 15.0).reshape(GROUPS, TOKG, HI * DI).astype(jnp.bfloat16)


def with_spikes(array, rng, source, target, blocks, factor):
    def block_of(dim):
        return (jnp.arange(array.shape[dim]) // (array.shape[dim] // blocks)).reshape((-1,) + (1,) * (array.ndim - 1 - dim))

    one_side = jax.random.permutation(rng, blocks)[block_of(target)]
    second = (block_of(target) + blocks // 2) % blocks
    return jnp.where((block_of(source) == one_side) | (block_of(source) == second), factor * array, array)


def shard_levels(own_key, shape, split, low, high):
    loudness, own = 1.0, jax.random.fold_in(own_key, 6)
    for axis_at, blocks in split:
        steps = jnp.exp(jax.random.uniform(jax.random.fold_in(own, axis_at), (blocks,), jnp.float32, low / len(split), high / len(split)))
        loudness = loudness * jnp.repeat(steps, shape[axis_at] // blocks).reshape([-1 if axis == axis_at else 1 for axis in range(len(shape))])
    return loudness


def length_profile(number_of, total, most, slope):
    loads = [(1 << 20) // math.isqrt(standing ** slope) + 1 for standing in range(2, number_of + 1)]
    surplus, given = total - most - (number_of - 1), [1] * (number_of - 1)
    while surplus > 0:
        candidates = [i for i in range(number_of - 1) if given[i] < most]
        mass, left = sum([loads[i] for i in candidates]), surplus
        for i in candidates:
            extra = min(most - given[i], max(1, left * loads[i] // mass), surplus)
            given[i] = given[i] + extra
            surplus = surplus - extra
    return np.array([most] + given)


def ragged(stream_key, amount, total, bound, lean):
    if amount == 2:
        one = jax.random.randint(stream_key, (), max(1, total - bound), min(bound, total - 1) + 1)
        return jnp.stack([one, total - one])
    tallies = jnp.asarray(length_profile(amount, total, bound, lean), jnp.int32)
    couples = (amount - 1) // 2
    giver, sink = tallies[1:1 + 2 * couples:2], tallies[2:2 + 2 * couples:2]
    slack = jnp.minimum(giver - 1, bound - sink)
    moved = jax.random.randint(jax.random.fold_in(stream_key, 1), (couples,), 0, 1 << 20) % (slack + 1)
    tallies = tallies.at[1:1 + 2 * couples:2].set(giver - moved).at[2:2 + 2 * couples:2].set(sink + moved)
    return tallies[jax.random.permutation(jax.random.fold_in(stream_key, 2), amount)]


def normal_values(own_key, dims, scale, most, pieces=(), kind=jnp.bfloat16):
    entries = scale * jax.random.normal(own_key, dims, jnp.float32)
    if pieces:
        entries = entries * shard_levels(own_key, dims, pieces, -0.22, 0.18)
    return jnp.clip(entries, -most, most).astype(kind)


def gaussian_with(rng, dims, spread, bound, split, heavy, held_as=jnp.bfloat16):
    values = spread * jax.random.normal(rng, dims, jnp.float32)
    if split:
        values = values * shard_levels(rng, dims, split, -0.22, 0.18)
    return jnp.clip(with_spikes(values, jax.random.fold_in(rng, 3), *heavy), -bound, bound).astype(held_as)


def setup_inputs(seed: int = 0) -> dict:
    key_of = jax.random.split(jax.random.key(seed), 8)
    return {
        "doc_lengths": jax.vmap(lambda own: ragged(own, DOCS, TOKG, DOC_MOST, 2))(jax.random.split(key_of[0], GROUPS)).reshape((GROUPS, DOCS)).astype(jnp.int32),
        "hidden": gaussian_with(key_of[1], (GROUPS, TOKG, D), 1.0, 6.0, ((0, 4), (1, 8)), (1, 2, 8, 2.0)),
        "gate_weight": normal_values(key_of[2], (D, HI), D ** -0.5, 0.0625, ((0, 32),)),
        "target_query": draw_target_query(jax.random.fold_in(key_of[7], 71), 0),
        "latent_keys": draw_latent_keys(jax.random.fold_in(key_of[7], 71), 0),
        "index_query": draw_index_query(jax.random.fold_in(key_of[7], 71), 0),
        "index_keys": draw_index_keys(jax.random.fold_in(key_of[7], 71), 0),
    }


target_scale = 0.07216878364870322
highest = lax.Precision.HIGHEST


def divergence_terms(target_q, index_q, gate_values, latent_win, index_win, query_pos, key_pos, query_start):
    batch_n, row_n = query_pos.shape
    latent_projection_weight = latent_win.shape[-1]
    index_w = index_win.shape[-1]
    target_heads = target_q.reshape(batch_n, row_n, -1, latent_projection_weight).astype(jnp.float32)
    indexer_head_weights = index_q.reshape(batch_n, row_n, -1, index_w).astype(jnp.float32)
    allowed = (key_pos[:, None, :] >= query_start[:, :, None]) & (key_pos[:, None, :] <= query_pos[:, :, None])
    logits = jnp.einsum("srhc,skc->srhk", target_heads, latent_win.astype(jnp.float32), precision=highest) * target_scale
    logits = jnp.where(allowed[:, :, None, :], logits, -jnp.inf)
    peak_value = jnp.max(logits, axis=-1, keepdims=True)
    exponent = jnp.exp(logits - peak_value)
    probabilities = exponent / jnp.sum(exponent, axis=-1, keepdims=True)
    target = jnp.mean(probabilities, axis=2)
    relu_score = jnp.maximum(jnp.einsum("srhd,skd->srhk", indexer_head_weights, index_win.astype(jnp.float32), precision=highest), 0.0)
    factor = index_w ** -0.5
    score = factor * jnp.einsum("srh,srhk->srk", gate_values, relu_score, precision=highest)
    masked = jnp.where(allowed, score, -jnp.inf)
    largest_value_seen = jnp.max(masked, axis=-1, keepdims=True)
    shifted = masked - largest_value_seen
    log_model = shifted - jnp.log(jnp.sum(jnp.exp(shifted), axis=-1, keepdims=True))
    log_model = jnp.where(allowed, log_model, 0.0)
    model_prob = jnp.where(allowed, jnp.exp(log_model), 0.0)
    positive = target > 0
    target_log_probabilities = jnp.where(positive, target * jnp.log(jnp.where(positive, target, 1.0)), 0.0)
    row_div = jnp.sum(jnp.where(allowed, target_log_probabilities - target * log_model, 0.0), axis=-1)
    delta_terms = factor * jnp.einsum("srk,srhk->srh", model_prob - target, relu_score, precision=highest)
    return row_div, delta_terms


def reference(doc_lengths, hidden, gate_weight, target_query, latent_keys, index_query, index_keys):
    outputs = []
    grad_total = jnp.zeros((D, HI), jnp.float32)
    for group_index in range(GROUPS):
        lengths = doc_lengths[group_index]
        doc_ends = jnp.cumsum(lengths)
        gates_all = jnp.dot(hidden[group_index], gate_weight, preferred_element_type=jnp.float32)
        latent_padding_rows = jnp.concatenate([jnp.zeros((DOC_MOST, RK), latent_keys.dtype), latent_keys[group_index]], 0)
        index_pad = jnp.concatenate([jnp.zeros((DOC_MOST, DI), index_keys.dtype), index_keys[group_index]], 0)
        target_group = target_query[group_index]
        index_group = index_query[group_index]

        def home_block(block_index):
            low_row = (block_index * TOK_DEV).astype(jnp.int32)
            query_pos = (low_row + jnp.arange(TOK_DEV, dtype=jnp.int32)).astype(jnp.int32)
            key_pos = (low_row - DOC_MOST + jnp.arange(WIN, dtype=jnp.int32)).astype(jnp.int32)
            query_start = jnp.sum(lengths[None, :] * (doc_ends[None, :] <= query_pos[:, None]).astype(jnp.int32), -1).astype(jnp.int32)
            target_rows = lax.dynamic_slice_in_dim(target_group, low_row, TOK_DEV, 0)
            index_rows = lax.dynamic_slice_in_dim(index_group, low_row, TOK_DEV, 0)
            gate_rows = lax.dynamic_slice_in_dim(gates_all, low_row, TOK_DEV, 0)
            latent_win = lax.dynamic_slice_in_dim(latent_padding_rows, low_row, WIN, 0)
            index_win = lax.dynamic_slice_in_dim(index_pad, low_row, WIN, 0)
            row_div, delta_terms = divergence_terms(target_rows[None], index_rows[None], gate_rows[None], latent_win[None], index_win[None], query_pos[None], key_pos[None], query_start[None])
            return row_div[0], delta_terms[0]

        row_div, delta_terms = lax.map(home_block, jnp.arange(N_SEQ, dtype=jnp.int32))
        outputs.append(row_div.reshape(TOKG))
        gate_delta = (delta_terms.reshape(TOKG, HI) / TOK_DEV).astype(jnp.bfloat16)
        grad_total = grad_total + jnp.dot(hidden[group_index].T, gate_delta, preferred_element_type=jnp.float32)
    return jnp.stack(outputs, 0), grad_total
```

```python
import functools
import math
import jax
import jax.numpy as jnp
from jax import lax
from jax.experimental import pallas as pl
from jax.experimental.pallas import tpu as pltpu
from jax.sharding import PartitionSpec as P

LOOK = 8
LANES = 128
CHUNK = 64

target_scale = 0.07216878364870322
log2e = 1.4426950408889634
floor_value = -1e30
NT = (((1,), (1,)), ((), ()))
TN = (((0,), (0,)), ((), ()))


def shifted(block, axis, distance):
    devices = range(lax.axis_size(axis))
    route = [(i - distance, i) for i in devices if i - distance in devices]
    return lax.ppermute(block, axis, route)


def bit_steps():
    steps = []
    for axis in ("seq", "grp"):
        size = lax.axis_size(axis)
        bit = size // 2
        while bit:
            steps.append((axis, bit))
            bit //= 2
    return steps


def swap(block, axis, bit):
    return lax.ppermute(block, axis, [(i, i ^ bit) for i in range(lax.axis_size(axis))])


def bit_of(axis, bit):
    return (lax.axis_index(axis) // bit) % 2


def reversed_bits(number, width):
    result = 0
    for _ in range(width):
        result = result * 2 + number % 2
        number //= 2
    return result


def row_window(lens_ref, first_row, panel_start, keys, rows):
    position = first_row + lax.broadcasted_iota(jnp.int32, (1, rows), 1)
    start = jnp.zeros((1, rows), jnp.int32)
    end = jnp.int32(0)
    for d in range(lens_ref.shape[0]):
        length = lens_ref[d]
        end = end + length
        start = start + jnp.where(position >= end, length, 0)

    def allowed(low, count):
        key = panel_start + low + lax.broadcasted_iota(jnp.int32, (count, rows), 0)
        return (key >= start) & (key <= position)

    return allowed


def fold8(value):
    return value.reshape(value.shape[0] // 8, 8, value.shape[1])


def target_kernel(reach, lens_ref, idx_ref, *refs):
    lat_refs = refs[: reach + 1]
    q_hbm, out_ref, q_v, ke, ko, sa, sb, bias, sem = refs[reach + 1 :]
    block = pl.program_id(0)
    rows = out_ref.shape[1]
    keys = out_ref.shape[0]
    width = lat_refs[0].shape[1]
    device_rows = lat_refs[0].shape[0]
    slab = ke.shape[1]
    pair = 2 * width
    pads = slab - width
    heads = q_v.shape[1] // width
    loops = heads // 4
    parts = sem.shape[0]
    part_cols = q_v.shape[1] // parts
    loops_per_part = loops // parts

    def part_copy(i):
        cols = pl.ds(pl.multiple_of(i * part_cols, LANES), part_cols)
        return pltpu.make_async_copy(
            q_hbm.at[pl.ds(pl.multiple_of(block * rows, rows), rows), cols], q_v.at[:, cols], sem.at[i]
        )

    for i in range(parts):
        part_copy(i).start()

    @pl.when(block == 0)
    def _():
        for i, lat in enumerate(lat_refs):
            spot = pl.ds(i * device_rows, device_rows)
            values = lat[...].astype(jnp.float32)
            wide = jnp.concatenate([values, jnp.zeros((device_rows, pads), jnp.float32)], 1)
            ke[spot, :] = wide.astype(jnp.bfloat16)
            ko[spot, :] = pltpu.roll(wide, pads, 1).astype(jnp.bfloat16)

    first_row = idx_ref[0] * device_rows + block * rows
    panel_start = (idx_ref[0] - reach) * device_rows
    allowed = row_window(lens_ref, first_row, panel_start, keys, rows)
    for low in range(0, keys, CHUNK):
        bias[pl.ds(low, CHUNK), :] = jnp.where(allowed(low, CHUNK), 0.0, floor_value)
        out_ref[pl.ds(low, CHUNK), :] = jnp.zeros((CHUNK, rows), jnp.float32)

    def logits(j, shift, panel, store):
        base = j * (2 * pair) + shift
        q0 = q_v[:, pl.ds(pl.multiple_of(base, LANES), slab)]
        q1 = q_v[:, pl.ds(pl.multiple_of(base + pair, LANES), slab)]
        both = jnp.concatenate([q0, q1], 0)
        value = lax.dot_general(panel[...], both, NT, preferred_element_type=jnp.float32)
        peak = jnp.full((8, 2 * rows), floor_value, jnp.float32)
        for low in range(0, keys, CHUNK):
            piece_bias = bias[pl.ds(low, CHUNK), :]
            piece = value[low : low + CHUNK] + jnp.concatenate([piece_bias, piece_bias], 1)
            store[pl.ds(low, CHUNK), :] = piece
            peak = jnp.maximum(peak, jnp.max(fold8(piece), 0))
        return jnp.max(peak, 0, keepdims=True)

    def softmax_add(store, peak):
        total = jnp.zeros((8, 2 * rows), jnp.float32)
        for low in range(0, keys, CHUNK):
            piece = jnp.exp2((store[pl.ds(low, CHUNK), :] - peak) * (target_scale * log2e))
            store[pl.ds(low, CHUNK), :] = piece
            total = total + jnp.sum(fold8(piece), 0)
        scale = 1.0 / (jnp.sum(total, 0, keepdims=True) * heads)
        for low in range(0, keys, CHUNK):
            piece = store[pl.ds(low, CHUNK), :] * scale
            out_ref[pl.ds(low, CHUNK), :] += piece[:, :rows] + piece[:, rows:]

    part_copy(0).wait()
    peak_a = logits(0, 0, ke, sa)

    def step(j, peak_a):
        peak_b = logits(j, pair - slab, ko, sb)
        softmax_add(sa, peak_a)
        after = jnp.minimum(j + 1, loops - 1)

        @pl.when((after % loops_per_part == 0) & (after > j))
        def _():
            part_copy(after // loops_per_part).wait()

        peak_a = logits(after, 0, ke, sa)
        softmax_add(sb, peak_b)
        return peak_a

    lax.fori_loop(0, loops, step, peak_a)


def target_call(lengths, index, lat_parts, queries):
    reach = len(lat_parts) - 1
    rows_all, cols = queries.shape
    width = lat_parts[0].shape[1]
    rows = LANES
    keys = (reach + 1) * rows_all
    slab = (width + LANES - 1) // LANES * LANES
    parts = 8
    return pl.pallas_call(
        functools.partial(target_kernel, reach),
        out_shape=jax.ShapeDtypeStruct((keys, rows_all), jnp.float32),
        grid_spec=pltpu.PrefetchScalarGridSpec(
            num_scalar_prefetch=2,
            grid=(rows_all // rows,),
            in_specs=[pl.BlockSpec((rows_all, width), lambda i, *_: (0, 0))] * (reach + 1)
            + [pl.BlockSpec(memory_space=pl.ANY)],
            out_specs=pl.BlockSpec((keys, rows), lambda i, *_: (0, i)),
            scratch_shapes=[
                pltpu.VMEM((rows, cols), jnp.bfloat16),
                pltpu.VMEM((keys, slab), jnp.bfloat16),
                pltpu.VMEM((keys, slab), jnp.bfloat16),
                pltpu.VMEM((keys, 2 * rows), jnp.float32),
                pltpu.VMEM((keys, 2 * rows), jnp.float32),
                pltpu.VMEM((keys, rows), jnp.float32),
                pltpu.SemaphoreType.DMA((parts,)),
            ],
        ),
        compiler_params=pltpu.CompilerParams(dimension_semantics=("arbitrary",)),
        cost_estimate=pl.CostEstimate(
            flops=2 * rows_all * cols * keys,
            bytes_accessed=rows_all * cols * 2,
            transcendentals=rows_all * cols // width * keys,
        ),
        name="target_terms",
    )(lengths, index, *lat_parts, queries)


def index_kernel(reach, bits, lens_ref, idx_ref, *refs):
    key_refs = refs[: reach + 1]
    (target_ref, hidden_ref, weight_ref, query_ref, div_ref, part_ref, panel, weight, gates, score, delta) = refs[
        reach + 1 :
    ]
    block = pl.program_id(0)
    keys, rows = target_ref.shape
    device_rows, width = key_refs[0].shape
    heads = query_ref.shape[1] // width
    blocks, block_rows, _ = weight_ref.shape
    half = blocks * block_rows
    factor = width ** (-0.5)
    unroll = 4

    @pl.when(block == 0)
    def _():
        for i, ref in enumerate(key_refs):
            panel[pl.ds(i * device_rows, device_rows), :] = ref[...]
        for i in range(blocks):
            weight[pl.ds(reversed_bits(i, bits) * block_rows, block_rows), :] = weight_ref[i]

    low_gates = jnp.dot(hidden_ref[:, :half], weight[...], preferred_element_type=jnp.float32)
    high_gates = jnp.dot(hidden_ref[:, half:], weight[...], preferred_element_type=jnp.float32)
    gates[...] = low_gates[:, :heads].T + high_gates[:, heads:].T
    for low in range(0, keys, CHUNK):
        score[pl.ds(low, CHUNK), :] = jnp.zeros((CHUNK, rows), jnp.float32)

    def relu_pair(h):
        q0 = query_ref[:, pl.ds(pl.multiple_of(h * width, LANES), width)]
        q1 = query_ref[:, pl.ds(pl.multiple_of((h + 1) * width, LANES), width)]
        both = jnp.concatenate([q0, q1], 0)
        return lax.dot_general(panel[...], both, NT, preferred_element_type=jnp.float32)

    def score_step(i, carry):
        for u in range(unroll):
            h = (i * unroll + u) * 2
            value = relu_pair(h)
            g0 = gates[pl.ds(h, 1), :]
            g1 = gates[pl.ds(h + 1, 1), :]
            for low in range(0, keys, CHUNK):
                piece = jnp.maximum(value[low : low + CHUNK], 0.0)
                score[pl.ds(low, CHUNK), :] += piece[:, :rows] * g0 + piece[:, rows:] * g1
        return carry

    lax.fori_loop(0, heads // (2 * unroll), score_step, 0)

    first_row = idx_ref[0] * device_rows + block * rows
    panel_start = (idx_ref[0] - reach) * device_rows
    allowed = row_window(lens_ref, first_row, panel_start, keys, rows)
    peak = jnp.full((8, rows), floor_value, jnp.float32)
    for low in range(0, keys, CHUNK):
        piece = jnp.where(allowed(low, CHUNK), score[pl.ds(low, CHUNK), :] * factor, floor_value)
        score[pl.ds(low, CHUNK), :] = piece
        peak = jnp.maximum(peak, jnp.max(fold8(piece), 0))
    peak = jnp.max(peak, 0, keepdims=True)
    total = jnp.zeros((8, rows), jnp.float32)
    for low in range(0, keys, CHUNK):
        total = total + jnp.sum(fold8(jnp.exp(score[pl.ds(low, CHUNK), :] - peak)), 0)
    normal = peak + jnp.log(jnp.sum(total, 0, keepdims=True))
    spread = jnp.zeros((8, rows), jnp.float32)
    for low in range(0, keys, CHUNK):
        mask = allowed(low, CHUNK)
        log_model = jnp.where(mask, score[pl.ds(low, CHUNK), :] - normal, 0.0)
        target = target_ref[pl.ds(low, CHUNK), :]
        positive = target > 0
        log_target = jnp.log(jnp.where(positive, target, 1.0))
        spread = spread + jnp.sum(fold8(target * (log_target - log_model)), 0)
        score[pl.ds(low, CHUNK), :] = jnp.where(mask, jnp.exp(log_model), 0.0) - target
    div_ref[...] = jnp.sum(spread, 0, keepdims=True)

    def delta_step(i, carry):
        for u in range(unroll):
            h = (i * unroll + u) * 2
            value = relu_pair(h)
            sum0 = jnp.zeros((8, rows), jnp.float32)
            sum1 = jnp.zeros((8, rows), jnp.float32)
            for low in range(0, keys, CHUNK):
                piece = jnp.maximum(value[low : low + CHUNK], 0.0)
                weight_piece = score[pl.ds(low, CHUNK), :]
                sum0 = sum0 + jnp.sum(fold8(piece[:, :rows] * weight_piece), 0)
                sum1 = sum1 + jnp.sum(fold8(piece[:, rows:] * weight_piece), 0)
            delta[pl.ds(h, 1), :] = jnp.sum(sum0, 0, keepdims=True)
            delta[pl.ds(h + 1, 1), :] = jnp.sum(sum1, 0, keepdims=True)
        return carry

    lax.fori_loop(0, heads // (2 * unroll), delta_step, 0)

    gate_delta = (delta[...] * factor / device_rows).T
    zero = jnp.zeros_like(gate_delta)
    low_delta = jnp.concatenate([gate_delta, zero], 1).astype(jnp.bfloat16)
    high_delta = jnp.concatenate([zero, gate_delta], 1).astype(jnp.bfloat16)
    step = math.lcm(LANES, block_rows)
    for low in range(0, half, step):
        value = lax.dot_general(
            hidden_ref[:, low : low + step], low_delta, TN, preferred_element_type=jnp.float32
        ) + lax.dot_general(
            hidden_ref[:, half + low : half + low + step], high_delta, TN, preferred_element_type=jnp.float32
        )
        for i in range(step // block_rows):
            spot = reversed_bits(low // block_rows + i, bits)
            piece = value[i * block_rows : (i + 1) * block_rows]

            @pl.when(block == 0)
            def _():
                part_ref[spot] = piece

            @pl.when(block > 0)
            def _():
                part_ref[spot] += piece


def index_call(lengths, index, key_parts, target, hidden, weight, queries):
    reach = len(key_parts) - 1
    rows_all, cols = queries.shape
    width = key_parts[0].shape[1]
    rows = LANES
    keys = target.shape[0]
    heads = cols // width
    blocks, block_rows, lanes = weight.shape
    bits = blocks.bit_length() - 1
    depth = hidden.shape[1]
    return pl.pallas_call(
        functools.partial(index_kernel, reach, bits),
        out_shape=(
            jax.ShapeDtypeStruct((1, rows_all), jnp.float32),
            jax.ShapeDtypeStruct(weight.shape, jnp.float32),
        ),
        grid_spec=pltpu.PrefetchScalarGridSpec(
            num_scalar_prefetch=2,
            grid=(rows_all // rows,),
            in_specs=[pl.BlockSpec((rows_all, width), lambda i, *_: (0, 0))] * (reach + 1)
            + [
                pl.BlockSpec((keys, rows), lambda i, *_: (0, i)),
                pl.BlockSpec((rows, depth), lambda i, *_: (i, 0)),
                pl.BlockSpec(weight.shape, lambda i, *_: (0, 0, 0)),
                pl.BlockSpec((rows, cols), lambda i, *_: (i, 0)),
            ],
            out_specs=(
                pl.BlockSpec((1, rows), lambda i, *_: (0, i)),
                pl.BlockSpec(weight.shape, lambda i, *_: (0, 0, 0)),
            ),
            scratch_shapes=[
                pltpu.VMEM((keys, width), jnp.bfloat16),
                pltpu.VMEM((blocks * block_rows, lanes), jnp.bfloat16),
                pltpu.VMEM((heads, rows), jnp.float32),
                pltpu.VMEM((keys, rows), jnp.float32),
                pltpu.VMEM((heads, rows), jnp.float32),
            ],
        ),
        compiler_params=pltpu.CompilerParams(dimension_semantics=("arbitrary",)),
        cost_estimate=pl.CostEstimate(
            flops=4 * rows_all * cols * keys + 4 * rows_all * depth * heads,
            bytes_accessed=rows_all * (cols + depth) * 2 + 2 * depth * heads * 4,
            transcendentals=2 * rows_all * keys,
        ),
        name="index_terms",
    )(lengths, index, *key_parts, target, hidden, weight, queries)


def body(doc_lengths, hidden, gate_weight, target_query, latent_keys, index_query, index_keys):
    seq_count = lax.axis_size("seq")
    my_index = lax.axis_index("seq")
    row_count = hidden.shape[1]
    reach = min(LOOK, seq_count // 2)
    lengths = doc_lengths[0]
    index = my_index.reshape(1).astype(jnp.int32)
    steps = bit_steps()

    lat_parts = [shifted(latent_keys[0], "seq", d) for d in range(reach, 0, -1)] + [latent_keys[0]]
    key_parts = [shifted(index_keys[0], "seq", d) for d in range(reach, 0, -1)] + [index_keys[0]]

    axis, bit = steps[0]
    other = swap(gate_weight, axis, bit)
    mine_high = bit_of(axis, bit) == 1
    weight = jnp.where(
        mine_high, jnp.concatenate([other, gate_weight], 1), jnp.concatenate([gate_weight, other], 1)
    )[None]
    for axis, bit in steps[1:]:
        other = swap(weight, axis, bit)
        mine_high = bit_of(axis, bit) == 1
        weight = jnp.where(
            mine_high, jnp.concatenate([other, weight], 0), jnp.concatenate([weight, other], 0)
        )

    target = target_call(lengths, index, lat_parts, target_query[0])
    divergence, part = index_call(lengths, index, key_parts, target, hidden[0], weight, index_query[0])

    for axis, bit in reversed(steps[1:]):
        count = part.shape[0] // 2
        mine = bit_of(axis, bit)
        keep = lax.dynamic_slice_in_dim(part, mine * count, count, 0)
        send = lax.dynamic_slice_in_dim(part, (1 - mine) * count, count, 0)
        part = keep + swap(send, axis, bit)
    part = part[0]
    heads = part.shape[1] // 2
    axis, bit = steps[0]
    mine_high = bit_of(axis, bit) == 1
    low, high = part[:, :heads], part[:, heads:]
    keep = jnp.where(mine_high, high, low)
    send = jnp.where(mine_high, low, high)
    grad_gate = keep + swap(send, axis, bit)
    return divergence, grad_gate


def solution(mesh):
    in_specs = (
        P("grp", None),
        P("grp", "seq", None),
        P(("seq", "grp"), None),
        P("grp", "seq", None),
        P("grp", "seq", None),
        P("grp", "seq", None),
        P("grp", "seq", None),
    )
    out_specs = (P("grp", "seq"), P(("seq", "grp"), None))
    return jax.shard_map(body, mesh=mesh, in_specs=in_specs, out_specs=out_specs, check_vma=False)
```
